32 devices in a mesh: gx: 4 (over y, x), gy: 2 (over core), gz: 4 (over z).
Axes of the slice: x: 2, y: 2, z: 4, core: 2. Of those that a mesh axis runs over, the one named last changes fastest.
Arguments:
- residual_in: float32 [256, 128, 1024], P('gx', 'gy', 'gz'), may hold values from -700 to 700
Outputs:
- level_one: float32 [128, 64, 512], P('gx', 'gy', 'gz')
- level_two: float32 [64, 32, 256], P('gx', 'gy', 'gz')
- level_three: float32 [32, 16, 128], P('gx', 'gy', 'gz')
- level_four: float32 [16, 8, 64], P('gx', 'gy', 'gz')
- level_five: float32 [8, 4, 32], P('gx', 'gy', 'gz')
- level_scales: float32 [5], replicated
The draws below stay inside these ranges and needn't reach their ends.
All inputs are finite; a program needn't handle non-finite values.
Results may differ from the reference program's by a relative error of at most 0.0002.
Values sent between devices are 32-bit elements; how exact they have to be, the bound alone decides.
A program may use at most 64 MiB of HBM per device.

```python
import math
import jax
import jax.numpy as jnp
from jax import lax

LEVELS = 5
NX = 256
NY = 128
NZ = 1024


def draw_residual_in(key, part):
    key_list = jax.random.split(key, 5)
    ramp_x = jnp.exp(0.5 * math.log(3.0) * jnp.arange(NX, dtype=jnp.float32) / max(NX - 1, 1))
    ramp_y = jnp.exp(0.5 * math.log(3.0) * jnp.arange(NY, dtype=jnp.float32) / max(NY - 1, 1))
    ramp_z = jnp.exp(0.5 * math.log(3.0) * jnp.arange(NZ, dtype=jnp.float32) / max(NZ - 1, 1))
    rough_x = jnp.exp(0.5 * math.log(10.0) * jax.random.uniform(key_list[0], (NX,), jnp.float32))
    rough_y = jnp.exp(0.5 * math.log(10.0) * jax.random.uniform(key_list[1], (NY,), jnp.float32))
    rough_z = jnp.exp(0.5 * math.log(10.0) * jax.random.uniform(key_list[2], (NZ,), jnp.float32))
    amplitude = (ramp_x * rough_x)[:, None, None] * (ramp_y * rough_y)[None, :, None] * (ramp_z * rough_z)[None, None, :]
    values = amplitude * jax.random.truncated_normal(key_list[4], -4.0, 4.0, (NX, NY, NZ), jnp.float32)
    return values.astype(jnp.float32)


def setup_inputs(seed: int = 0) -> dict:
    arg_keys = jax.random.split(jax.random.key(seed), 2)
    residual_in = draw_residual_in(jax.random.fold_in(arg_keys[1], 71), 0)
    return {"residual_in": residual_in}


WEIGHTS = (0.25, 0.5, 0.25)
EPSILON = 1e-06

def restrict_cube(values):
    half_x = values.shape[0] // 2
    half_y = values.shape[1] // 2
    half_z = values.shape[2] // 2
    padded = jnp.pad(values, ((1, 0), (1, 0), (1, 0)))
    summed = jnp.zeros((half_x, half_y, half_z), jnp.float32)
    for off_x in range(3):
        for off_y in range(3):
            for off_z in range(3):
                picked = lax.slice(padded, (off_x, off_y, off_z), (off_x + 2 * half_x - 1, off_y + 2 * half_y - 1, off_z + 2 * half_z - 1), (2, 2, 2))
                summed = summed + WEIGHTS[off_x] * WEIGHTS[off_y] * WEIGHTS[off_z] * picked
    return summed

def reference(residual_in):
    current = residual_in
    grid_list = []
    scale_list = []
    for step_no in range(LEVELS):
        coarse = restrict_cube(current)
        mean_sq = jnp.sum(coarse * coarse) / coarse.size
        scale_now = jnp.sqrt(mean_sq + EPSILON)
        current = coarse / scale_now
        grid_list.append(current)
        scale_list.append(scale_now)
    return (grid_list[0], grid_list[1], grid_list[2], grid_list[3], grid_list[4], jnp.stack(scale_list))
```

```python
import functools

import jax
import jax.numpy as jnp
import ml_dtypes
import numpy as np
from jax import lax
from jax.experimental import pallas as pl
from jax.experimental.pallas import tpu as pltpu
from jax.sharding import PartitionSpec as P

LEVELS = 5
EPSILON = 1e-06
LANES = 128
AXES = ("gx", "gy", "gz")
MESH = pl.DeviceIdType.MESH
HOPS = ((1, 0, 0), (0, 1, 0), (1, 1, 0), (0, 0, 1), (1, 0, 1), (0, 1, 1), (1, 1, 1))


def round_up(n, m):
    return -(-n // m) * m


def step_matrix(n_in, n_cells):
    out = np.zeros((n_cells // 2 + 1, n_in))
    for i in range(n_cells // 2 + 1):
        for off, w in ((-1, 0.25), (0, 0.5), (1, 0.25)):
            if 0 <= 2 * i + off < n_in:
                out[i, 2 * i + off] = w
    return out


def composites(cells):
    mats, m, n = [], None, cells // 2
    for _ in range(LEVELS - 1):
        s = step_matrix(n + 1, n)
        m = s if m is None else s @ m
        mats.append(m)
        n //= 2
    return mats


def exact(table):
    out = table.astype(np.float32).astype(ml_dtypes.bfloat16)
    assert (out.astype(np.float64) == table).all()
    return out


class Plan:
    def __init__(self, shape):
        self.nx, self.ny, self.nz = shape
        self.x1, self.y1, self.z1 = (n // 2 for n in shape)
        assert self.z1 == LANES and self.y1 % 8 == 0
        self.xs = [self.nx >> l for l in range(2, LEVELS + 1)]
        self.ys = [self.ny >> l for l in range(2, LEVELS + 1)]
        self.zs = [self.nz >> l for l in range(2, LEVELS + 1)]
        self.pys = [round_up(y, 8) for y in self.ys]
        self.pxs = [round_up(x, 8) for x in self.xs]
        self.base = np.concatenate([[0], np.cumsum([x * p for x, p in zip(self.xs, self.pys)])]).tolist()
        self.own = round_up(self.base[-1], LANES)
        self.xoff = np.concatenate([[0], np.cumsum(self.pys)]).tolist()
        self.yoff = np.concatenate([[0], np.cumsum(self.pxs)]).tolist()
        self.bx = max(self.y1, self.xoff[-1])
        self.by = max(self.x1, self.yoff[-1])
        self.y0 = self.bx
        self.c0 = self.bx + self.by
        assert self.c0 + 8 <= LANES and self.x1 <= LANES
        self.coff = np.concatenate([[0], np.cumsum(self.zs)]).tolist()
        assert self.coff[-1] <= LANES
        self.main = self.x1 * self.y1
        self.rows1 = self.main + LANES
        self.crows = self.own + LANES

    def row1(self, i, j):
        if i < self.x1 and j < self.y1:
            return i * self.y1 + j
        if j < self.y1:
            return self.main + j
        if i < self.x1:
            return self.main + self.y0 + i
        return self.main + self.c0

    def tables(self):
        xm, ym, zm = composites(self.nx), composites(self.ny), composites(self.nz)
        order = np.array([[self.row1(i, j) for j in range(self.y1 + 1)] for i in range(self.x1 + 1)])
        big = np.zeros((self.crows, self.rows1))
        spread = np.zeros((self.own, LANES))
        for l in range(LEVELS - 1):
            nx, ny = self.xs[l], self.ys[l]
            for i in range(nx + 1):
                for j in range(ny + 1):
                    if i < nx and j < ny:
                        r = self.base[l] + i * self.pys[l] + j
                    elif j < ny:
                        r = self.own + self.xoff[l] + j
                    elif i < nx:
                        r = self.own + self.y0 + self.yoff[l] + i
                    else:
                        r = self.own + self.c0 + l
                    big[r, order] = xm[l][i][:, None] * ym[l][j][None, :]
            for j in range(ny):
                spread[self.base[l] + j, self.xoff[l] + j] = 1
            for i in range(nx):
                spread[self.base[l] + i * self.pys[l], self.y0 + self.yoff[l] + i] = 1
            spread[self.base[l], self.c0 + l] = 1
        z_first = step_matrix(self.nz, self.nz)
        kz1 = np.zeros((self.nz, 2 * LANES))
        kz1[:, :LANES] = z_first[:LANES].T
        kz1[:, LANES:] = z_first[LANES][:, None]
        kz = np.zeros((2 * LANES, LANES))
        tails = np.zeros((16, 2 * LANES))
        place = np.zeros((16, 2 * LANES))
        for l in range(LEVELS - 1):
            kz[: LANES + 1, self.coff[l] : self.coff[l + 1]] = zm[l][:-1].T
            tails[l, : LANES + 1] = zm[l][-1]
            place[l, LANES + self.coff[l]] = 1
        tail1 = np.zeros((16, self.nz))
        tail1[LEVELS - 1] = z_first[LANES]
        place[LEVELS - 1, 0] = 1
        return [exact(t) for t in (kz1, kz, tails, tail1, place, spread, big)]


def halves(x):
    hi = x.astype(jnp.bfloat16)
    return hi, (x - hi.astype(jnp.float32)).astype(jnp.bfloat16)


def dot(a, b, dims=((1,), (0,))):
    return lax.dot_general(a, b, (dims, ((), ())), preferred_element_type=jnp.float32)


def gather_kernel(plan, sizes, chunks, *refs):
    p = plan
    v_hbm, *tabs_hbm = refs[:8]
    out1, outc, stats = refs[8:11]
    (vin, planes, spill, uhi, ulo, z, zhi, zlo, dacc) = refs[11:20]
    tabs = refs[20:27]
    sends = refs[27:32]
    recvs = refs[32:37]
    mine, parts, vsem, tsem, ssem, rsem, assem, arsem = refs[37:45]
    kz1, kz, tails, tail1, place, spread, big = tabs
    pos = [lax.axis_index(a) for a in AXES]
    count = sizes[0] * sizes[1] * sizes[2]
    me = (pos[0] * sizes[1] + pos[1]) * sizes[2] + pos[2]

    def coords(r):
        return {
            "gx": r // (sizes[1] * sizes[2]),
            "gy": (r // sizes[2]) % sizes[1],
            "gz": r % sizes[2],
        }

    barrier = pltpu.get_barrier_semaphore()

    @pl.loop(1, count)
    def _(k):
        pl.semaphore_signal(
            barrier, inc=1, device_id=coords(lax.rem(me + k, count)), device_id_type=MESH
        )

    per = p.nx // chunks
    tcopies = [
        pltpu.make_async_copy(tabs_hbm[i], tabs[i], tsem.at[i]) for i in range(7)
    ]
    vcopies = [
        pltpu.make_async_copy(
            v_hbm.at[pl.ds(c * per, per)], vin.at[pl.ds(1 + c * per, per)], vsem.at[c]
        )
        for c in range(chunks)
    ]
    for i in range(6):
        tcopies[i].start()
    for c in vcopies:
        c.start()
    tcopies[6].start()

    half = per // 2
    vin[0] = jnp.zeros((p.ny, p.nz), jnp.float32)
    lanes = lax.broadcasted_iota(jnp.int32, (p.y1, LANES), 1)
    spill[...] = jnp.zeros_like(spill)
    for j in range(half):
        planes[j, :, 0:8, :] = jnp.zeros((2, 8, LANES), jnp.float32)
    dacc[...] = jnp.zeros_like(dacc)
    for i in range(6):
        tcopies[i].wait()

    def fold_y(j):
        cols = []
        for h in range(2):
            even = planes[j, h, pl.ds(8, p.y1, 2), :]
            odd = planes[j, h, pl.ds(9, p.y1, 2), :]
            prev = planes[j, h, pl.ds(7, p.y1, 2), :]
            cols.append(0.5 * even + 0.25 * (odd + prev))
        return jnp.concatenate(cols, axis=1)

    def last_y(j):
        end = 8 + p.ny
        return jnp.concatenate(
            [0.25 * planes[j, h, end - 1 : end, :] for h in range(2)], axis=1
        )

    def put_plane(j, t):
        for h in range(2):
            planes[j, h, 8:, :] = t[:, h * LANES : (h + 1) * LANES]

    for c in range(chunks):
        vcopies[c].wait()

        @pl.loop(0, half)
        def _(j):
            i = c * half + j
            put_plane(j, 0.5 * vin[2 * i + 1] + 0.25 * (vin[2 * i + 2] + vin[2 * i]))
            hi, lo = halves(fold_y(j))
            rows = pl.ds(pl.multiple_of(i * p.y1, p.y1), p.y1)
            uhi[rows, :] = hi
            ulo[rows, :] = lo
            spill[pl.ds(p.y0 + i, 1), :] = last_y(j)

        rows = pl.ds(c * half * p.y1, half * p.y1)
        z[rows, :] = dot(uhi[rows, :], kz1[...]) + dot(ulo[rows, :], kz1[...])

        @pl.loop(0, half)
        def _(j):
            i = c * half + j
            rows = pl.ds(pl.multiple_of(i * p.y1, p.y1), p.y1)
            plane = z[rows, :]
            dacc[...] += jnp.where(lanes == i, plane[:, LANES:], 0.0)
            hi, lo = halves(plane)
            zhi[rows, :] = hi
            zlo[rows, :] = lo

    put_plane(0, 0.25 * vin[p.nx])
    spill[0 : p.y1, :] = fold_y(0)
    spill[p.c0 : p.c0 + 1, :] = last_y(0)
    shi, slo = halves(spill[...])
    zs = dot(shi, kz1[...]) + dot(slo, kz1[...])
    hi, lo = halves(zs)
    zhi[p.main :, :] = hi
    zlo[p.main :, :] = lo
    tail_one = dot(tail1[...], shi, ((1,), (1,))) + dot(tail1[...], slo, ((1,), (1,)))
    tcopies[6].wait()
    b = dot(big[...], zhi[...]) + dot(big[...], zlo[...])
    bhi, blo = halves(b)
    cs = dot(bhi, kz[...]) + dot(blo, kz[...])
    tail_c = dot(tails[...], bhi, ((1,), (1,))) + dot(tails[...], blo, ((1,), (1,)))

    mx, my, mxy, mz, m8 = sends
    mx[0 : p.bx, :] = zs[0 : p.bx, :LANES]
    mx[p.bx :, :] = cs[p.own : p.own + p.bx]
    my[0 : p.by, :] = zs[p.y0 : p.c0, :LANES]
    my[p.by :, :] = cs[p.own + p.y0 : p.own + p.c0]
    mxy[0:8, :] = zs[p.c0 : p.c0 + 8, :LANES]
    mxy[8:16, :] = cs[p.own + p.c0 : p.own + p.c0 + 8]
    mz[0 : p.y1, :] = dacc[...]
    groups = p.own // LANES
    for g in range(groups):
        mz[p.y1 + 8 * g : p.y1 + 8 * g + 8, :] = tail_c[0:8, g * LANES : (g + 1) * LANES]
    m8[...] = tail_one[0:8] + tail_c[0:8, p.own :]

    pl.semaphore_wait(barrier, count - 1)

    rx, ry, rxy, rz, r8 = recvs
    srcs = [mx, my, mxy, mz, m8, m8, m8]
    dsts = [rx, ry, rxy, rz, r8.at[0], r8.at[1], r8.at[2]]
    has_next, has_prev, copies = [], [], []
    for n, hop in enumerate(HOPS):
        ok_n, ok_p = True, True
        target = {}
        for a in range(3):
            if hop[a]:
                ok_n = jnp.logical_and(ok_n, pos[a] < sizes[a] - 1)
                ok_p = jnp.logical_and(ok_p, pos[a] > 0)
                target[AXES[a]] = lax.rem(pos[a] + 1, sizes[a])
            else:
                target[AXES[a]] = pos[a]
        has_next.append(ok_n)
        has_prev.append(ok_p)
        copies.append(
            pltpu.make_async_remote_copy(
                src_ref=srcs[n],
                dst_ref=dsts[n],
                send_sem=ssem.at[n],
                recv_sem=rsem.at[n],
                device_id=target,
                device_id_type=MESH,
            )
        )
    for n in (3, 0, 1, 2, 4, 5, 6):

        @pl.when(has_next[n])
        def _():
            copies[n].start()

    for n in range(7):

        @pl.when(has_prev[n])
        def _():
            copies[n].wait_recv()

        @pl.when(jnp.logical_not(has_prev[n]))
        def _():
            dsts[n][...] = jnp.zeros(dsts[n].shape, jnp.float32)

    lane8 = lax.broadcasted_iota(jnp.int32, (8, LANES), 1)
    g8 = jnp.where(lane8 < p.y0, r8[0], jnp.where(lane8 < p.c0, r8[1], r8[2]))

    def turned(x, where):
        hi, lo = halves(x.T)
        return dot(hi, where) + dot(lo, where)

    f = turned(g8, place[0:8, :])
    xs1 = rx[0 : p.bx, :] + f[0 : p.bx, :LANES]
    ys1 = ry[0 : p.by, :] + f[p.y0 : p.c0, :LANES]
    xy1 = rxy[0:8, :] + f[p.c0 : p.c0 + 8, :LANES]
    pieces = [
        rx[p.bx :, :] + f[0 : p.bx, LANES:],
        ry[p.by :, :] + f[p.y0 : p.c0, LANES:],
        rxy[8:16, :] + f[p.c0 : p.c0 + 8, LANES:],
    ]
    if p.c0 + 8 < LANES:
        pieces.append(jnp.zeros((LANES - p.c0 - 8, LANES), jnp.float32))
    whi, wlo = halves(jnp.concatenate(pieces, axis=0))
    c = cs[0 : p.own] + dot(spread[...], whi) + dot(spread[...], wlo)
    c = c + jnp.concatenate(
        [
            turned(rz[p.y1 + 8 * g : p.y1 + 8 * g + 8, :], place[0:8, LANES:])
            for g in range(groups)
        ],
        axis=0,
    )
    outc[...] = c

    first = lanes == 0
    top = lax.broadcasted_iota(jnp.int32, (p.y1, LANES), 0) == 0
    col = rz[0 : p.y1, :]
    acc = jnp.zeros((p.y1, LANES), jnp.float32)
    for i in range(p.x1):
        shifted = pltpu.roll(col, (LANES - i) % LANES, 1) if i else col
        plane = z[i * p.y1 : (i + 1) * p.y1, :LANES] + jnp.where(first, shifted, 0.0)
        edge = ys1[i : i + 1, :]
        if i == 0:
            plane = plane + xs1[0 : p.y1]
            edge = edge + xy1[0:1, :]
        plane = plane + jnp.where(top, edge, 0.0)
        out1[i] = plane
        acc = acc + plane * plane
    mine[0:1, :] = jnp.sum(acc, axis=0, keepdims=True)
    sq = c * c
    lane1 = lax.broadcasted_iota(jnp.int32, (1, LANES), 1)
    row = jnp.zeros((1, LANES), jnp.float32)
    for l in range(LEVELS - 1):
        total = jnp.sum(sq[p.base[l] : p.base[l + 1]], axis=0, keepdims=True)
        row = jnp.where((lane1 >= p.coff[l]) & (lane1 < p.coff[l + 1]), total, row)
    mine[1:2, :] = row

    def part(k):
        return pltpu.make_async_remote_copy(
            src_ref=mine,
            dst_ref=parts.at[k],
            send_sem=assem.at[k],
            recv_sem=arsem.at[k],
            device_id=coords(lax.rem(me + k, count)),
            device_id_type=MESH,
        )

    @pl.loop(1, count)
    def _(k):
        part(k).start()

    parts[0] = mine[...]

    for n in range(7):

        @pl.when(has_next[n])
        def _():
            copies[n].wait_send()

    @pl.loop(1, count)
    def _(k):
        part(k).wait_recv()

    stats[...] = jnp.sum(parts[...], axis=0)

    @pl.loop(1, count)
    def _(k):
        part(k).wait_send()


def scale_kernel(plan, devices, grid, packed, stats, o1, o2, o3, o4, o5, scales):
    p = plan
    lane1 = lax.broadcasted_iota(jnp.int32, (1, LANES), 1)
    outs = (o1, o2, o3, o4, o5)
    product = jnp.ones((1, 1), jnp.float32)
    for l in range(LEVELS):
        row = stats[0:1, :] if l == 0 else stats[1:2, :]
        if l:
            row = jnp.where(
                (lane1 >= p.coff[l - 1]) & (lane1 < p.coff[l]), row, 0.0
            )
        total = jnp.sum(row, axis=1, keepdims=True)
        cells = devices * (p.nx >> (l + 1)) * (p.ny >> (l + 1)) * (p.nz >> (l + 1))
        scale = jnp.sqrt(total / (product * product) / cells + EPSILON)
        product = product * scale
        scales[l] = scale[0, 0]
        inverse = 1.0 / product
        if l == 0:
            o1[...] = grid[...] * inverse.reshape(1, 1, 1)
            continue
        k = l - 1
        block = packed[p.base[k] : p.base[k + 1], :] * inverse
        if p.coff[k]:
            block = pltpu.roll(block, LANES - p.coff[k], 1)
        block = block.reshape(p.xs[k], p.pys[k], LANES)
        outs[l][...] = block[:, : p.ys[k], : p.zs[k]]


def per_device(sizes, residual_in):
    plan = Plan(residual_in.shape)
    p = plan
    tables = p.tables()
    chunks = 4
    count = sizes[0] * sizes[1] * sizes[2]
    f32, bf16 = jnp.float32, jnp.bfloat16
    messages = [
        (2 * p.bx, LANES),
        (2 * p.by, LANES),
        (16, LANES),
        (p.y1 + 8 * (p.own // LANES), LANES),
    ]
    anywhere = pl.BlockSpec(memory_space=pl.ANY)
    vmem = pl.BlockSpec(memory_space=pltpu.VMEM)
    dma = pltpu.SemaphoreType.DMA
    grid, packed, stats = pl.pallas_call(
        functools.partial(gather_kernel, p, sizes, chunks),
        out_shape=(
            jax.ShapeDtypeStruct((p.x1, p.y1, p.z1), f32),
            jax.ShapeDtypeStruct((p.own, LANES), f32),
            jax.ShapeDtypeStruct((2, LANES), f32),
        ),
        in_specs=[anywhere] * 8,
        out_specs=(vmem, vmem, vmem),
        scratch_shapes=[
            pltpu.VMEM((p.nx + 1, p.ny, p.nz), f32),
            pltpu.VMEM((p.nx // chunks // 2, 2, 8 + p.ny, LANES), f32),
            pltpu.VMEM((LANES, p.nz), f32),
            pltpu.VMEM((p.main, p.nz), bf16),
            pltpu.VMEM((p.main, p.nz), bf16),
            pltpu.VMEM((p.main, 2 * LANES), f32),
            pltpu.VMEM((p.rows1, 2 * LANES), bf16),
            pltpu.VMEM((p.rows1, 2 * LANES), bf16),
            pltpu.VMEM((p.y1, LANES), f32),
        ]
        + [pltpu.VMEM(t.shape, bf16) for t in tables]
        + [pltpu.VMEM(s, f32) for s in messages + [(8, LANES)]]
        + [pltpu.VMEM(s, f32) for s in messages + [(3, 8, LANES)]]
        + [
            pltpu.VMEM((2, LANES), f32),
            pltpu.VMEM((count, 2, LANES), f32),
            dma((chunks,)),
            dma((7,)),
            dma((7,)),
            dma((7,)),
            dma((count,)),
            dma((count,)),
        ],
        compiler_params=pltpu.CompilerParams(collective_id=0, has_side_effects=True),
        name="restrict_exchange",
    )(residual_in, *[jnp.asarray(t) for t in tables])
    shapes = [
        (p.nx >> l, p.ny >> l, p.nz >> l) for l in range(1, LEVELS + 1)
    ]
    return pl.pallas_call(
        functools.partial(scale_kernel, p, count),
        out_shape=tuple(jax.ShapeDtypeStruct(s, f32) for s in shapes)
        + (jax.ShapeDtypeStruct((LEVELS,), f32),),
        in_specs=[vmem] * 3,
        out_specs=(vmem,) * 5 + (pl.BlockSpec(memory_space=pltpu.SMEM),),
        name="scale_levels",
    )(grid, packed, stats)


def solution(mesh):
    sizes = tuple(mesh.shape[a] for a in AXES)
    spec = P(*AXES)
    return jax.shard_map(
        functools.partial(per_device, sizes),
        mesh=mesh,
        in_specs=(spec,),
        out_specs=(spec,) * 5 + (P(),),
        check_vma=False,
    )
```

```python
import functools

import jax
import jax.numpy as jnp
import ml_dtypes
import numpy as np
from jax import lax
from jax.experimental import pallas as pl
from jax.experimental.pallas import tpu as pltpu
from jax.sharding import PartitionSpec as P

LEVELS = 5
EPSILON = 1e-06
LANES = 128
AXES = ("gx", "gy", "gz")
MESH = pl.DeviceIdType.MESH
HOPS = ((1, 0, 0), (0, 1, 0), (1, 1, 0), (0, 0, 1), (1, 0, 1), (0, 1, 1), (1, 1, 1))


def round_up(n, m):
    return -(-n // m) * m


def step_matrix(n_in, n_cells):
    out = np.zeros((n_cells // 2 + 1, n_in))
    for i in range(n_cells // 2 + 1):
        for off, w in ((-1, 0.25), (0, 0.5), (1, 0.25)):
            if 0 <= 2 * i + off < n_in:
                out[i, 2 * i + off] = w
    return out


def composites(cells):
    mats, m, n = [], None, cells // 2
    for _ in range(LEVELS - 1):
        s = step_matrix(n + 1, n)
        m = s if m is None else s @ m
        mats.append(m)
        n //= 2
    return mats


def exact(table):
    out = table.astype(np.float32).astype(ml_dtypes.bfloat16)
    assert (out.astype(np.float64) == table).all()
    return out


class Plan:
    def __init__(self, shape):
        self.nx, self.ny, self.nz = shape
        self.x1, self.y1, self.z1 = (n // 2 for n in shape)
        assert self.z1 == LANES and self.y1 % 8 == 0
        self.xs = [self.nx >> l for l in range(2, LEVELS + 1)]
        self.ys = [self.ny >> l for l in range(2, LEVELS + 1)]
        self.zs = [self.nz >> l for l in range(2, LEVELS + 1)]
        self.pys = [round_up(y, 8) for y in self.ys]
        self.pxs = [round_up(x, 8) for x in self.xs]
        self.base = np.concatenate([[0], np.cumsum([x * p for x, p in zip(self.xs, self.pys)])]).tolist()
        self.own = round_up(self.base[-1], LANES)
        self.xoff = np.concatenate([[0], np.cumsum(self.pys)]).tolist()
        self.yoff = np.concatenate([[0], np.cumsum(self.pxs)]).tolist()
        self.bx = max(self.y1, self.xoff[-1])
        self.by = max(self.x1, self.yoff[-1])
        self.y0 = self.bx
        self.c0 = self.bx + self.by
        assert self.c0 + 8 <= LANES and self.x1 <= LANES
        self.coff = np.concatenate([[0], np.cumsum(self.zs)]).tolist()
        assert self.coff[-1] <= LANES
        self.main = self.x1 * self.y1
        self.rows1 = self.main + LANES
        self.crows = self.own + LANES

    def row1(self, i, j):
        if i < self.x1 and j < self.y1:
            return i * self.y1 + j
        if j < self.y1:
            return self.main + j
        if i < self.x1:
            return self.main + self.y0 + i
        return self.main + self.c0

    def tables(self):
        xm, ym, zm = composites(self.nx), composites(self.ny), composites(self.nz)
        order = np.array([[self.row1(i, j) for j in range(self.y1 + 1)] for i in range(self.x1 + 1)])
        big = np.zeros((self.crows, self.rows1))
        spread = np.zeros((self.own, LANES))
        for l in range(LEVELS - 1):
            nx, ny = self.xs[l], self.ys[l]
            for i in range(nx + 1):
                for j in range(ny + 1):
                    if i < nx and j < ny:
                        r = self.base[l] + i * self.pys[l] + j
                    elif j < ny:
                        r = self.own + self.xoff[l] + j
                    elif i < nx:
                        r = self.own + self.y0 + self.yoff[l] + i
                    else:
                        r = self.own + self.c0 + l
                    big[r, order] = xm[l][i][:, None] * ym[l][j][None, :]
            for j in range(ny):
                spread[self.base[l] + j, self.xoff[l] + j] = 1
            for i in range(nx):
                spread[self.base[l] + i * self.pys[l], self.y0 + self.yoff[l] + i] = 1
            spread[self.base[l], self.c0 + l] = 1
        z_first = step_matrix(self.nz, self.nz)
        kz1 = np.zeros((self.nz, 2 * LANES))
        kz1[:, :LANES] = z_first[:LANES].T
        kz1[:, LANES:] = z_first[LANES][:, None]
        kz = np.zeros((2 * LANES, LANES))
        tails = np.zeros((16, 2 * LANES))
        place = np.zeros((16, 2 * LANES))
        for l in range(LEVELS - 1):
            kz[: LANES + 1, self.coff[l] : self.coff[l + 1]] = zm[l][:-1].T
            tails[l, : LANES + 1] = zm[l][-1]
            place[l, LANES + self.coff[l]] = 1
        tail1 = np.zeros((16, self.nz))
        tail1[LEVELS - 1] = z_first[LANES]
        place[LEVELS - 1, 0] = 1
        return self.pack([kz1, kz, tails, tail1, place, spread], big)

    def pack(self, small, big):
        blocks = -(-self.rows1 // self.nz)
        rows = [np.zeros((self.crows, self.nz)) for _ in range(blocks)]
        for n, block in enumerate(rows):
            part = big[:, n * self.nz : (n + 1) * self.nz]
            block[:, : part.shape[1]] = part
        self.places, self.small = [], []
        at = blocks * self.crows
        for t in small:
            block = np.zeros((t.shape[0], self.nz))
            block[:, : t.shape[1]] = t
            rows.append(block)
            self.places.append((at, 0))
            self.small.append(t.shape)
            at += t.shape[0]
        return exact(np.concatenate(rows))


def halves(x):
    hi = x.astype(jnp.bfloat16)
    return hi, (x - hi.astype(jnp.float32)).astype(jnp.bfloat16)


def dot(a, b, dims=((1,), (0,))):
    return lax.dot_general(a, b, (dims, ((), ())), preferred_element_type=jnp.float32)


def gather_kernel(plan, sizes, chunks, *refs):
    p = plan
    v_hbm, packed_hbm = refs[:2]
    out1_hbm, outc_hbm, stats = refs[2:5]
    (vin, planes, spill, uhi, ulo, z, zhi, zlo, dacc) = refs[5:14]
    tabs = refs[14:21]
    sends = refs[21:30]
    recvs = refs[30:39]
    mine, parts = refs[39:41]
    vsem, tsem, bsem, ssem, rsem, asend, arecv = refs[41:48]
    out1, outc, osem = refs[48:51]
    kz1, kz, tails, tail1, place, spread, big = tabs
    pos = [lax.axis_index(a) for a in AXES]
    group = sizes[0] * sizes[1]
    me = pos[0] * sizes[1] + pos[1]

    in_plane = []
    for k in range(group):
        r = lax.rem(me + k, group)
        in_plane.append((r // sizes[1], lax.rem(r, sizes[1])))
    in_line = [lax.rem(pos[2] + k, sizes[2]) for k in range(sizes[2])]
    others = [
        {"gx": gx, "gy": gy, "gz": gz} for gz in in_line for gx, gy in in_plane
    ][1:]

    def along(hop, way):
        ok, target = None, {}
        for a in range(3):
            target[AXES[a]] = pos[a]
            if hop[a]:
                here = pos[a] < sizes[a] - 1 if way > 0 else pos[a] > 0
                ok = here if ok is None else jnp.logical_and(ok, here)
                target[AXES[a]] = lax.rem(pos[a] + way + sizes[a], sizes[a])
        return ok, target

    per = p.nx // chunks
    tcopies = [
        pltpu.make_async_copy(
            packed_hbm.at[pl.ds(at, t.shape[0]), pl.ds(lane, t.shape[1])], t, tsem.at[n]
        )
        for n, (t, (at, lane)) in enumerate(zip(tabs[:6], p.places))
    ]
    blocks = -(-p.rows1 // p.nz)
    bcopies = []
    for n in range(blocks):
        width = min(p.nz, p.rows1 - n * p.nz)
        bcopies.append(
            pltpu.make_async_copy(
                packed_hbm.at[pl.ds(n * p.crows, p.crows), pl.ds(0, width)],
                big.at[:, pl.ds(n * p.nz, width)],
                bsem.at[n],
            )
        )
    vcopies = [
        pltpu.make_async_copy(
            v_hbm.at[pl.ds(c * per, per)], vin.at[pl.ds(1 + c * per, per)], vsem.at[c]
        )
        for c in range(chunks)
    ]
    vcopies[0].start()
    for c in tcopies + vcopies[1:] + bcopies:
        c.start()

    barrier = pltpu.get_barrier_semaphore()
    for target in others:
        pl.semaphore_signal(barrier, inc=1, device_id=target, device_id_type=MESH)

    half = per // 2
    vin[0] = jnp.zeros((p.ny, p.nz), jnp.float32)
    lanes = lax.broadcasted_iota(jnp.int32, (p.y1, LANES), 1)
    spill[...] = jnp.zeros_like(spill)
    for j in range(half):
        planes[j, :, 0:8, :] = jnp.zeros((2, 8, LANES), jnp.float32)
    dacc[...] = jnp.zeros_like(dacc)
    for i in range(6):
        tcopies[i].wait()

    def fold_y(j):
        cols = []
        for h in range(2):
            even = planes[j, h, pl.ds(8, p.y1, 2), :]
            odd = planes[j, h, pl.ds(9, p.y1, 2), :]
            prev = planes[j, h, pl.ds(7, p.y1, 2), :]
            cols.append(0.5 * even + 0.25 * (odd + prev))
        return jnp.concatenate(cols, axis=1)

    def last_y(j):
        end = 8 + p.ny
        return jnp.concatenate(
            [0.25 * planes[j, h, end - 1 : end, :] for h in range(2)], axis=1
        )

    def put_plane(j, t):
        for h in range(2):
            planes[j, h, 8:, :] = t[:, h * LANES : (h + 1) * LANES]

    for c in range(chunks):
        vcopies[c].wait()

        @pl.loop(0, half)
        def _(j):
            i = c * half + j
            put_plane(j, 0.5 * vin[2 * i + 1] + 0.25 * (vin[2 * i + 2] + vin[2 * i]))
            hi, lo = halves(fold_y(j))
            rows = pl.ds(pl.multiple_of(i * p.y1, p.y1), p.y1)
            uhi[rows, :] = hi
            ulo[rows, :] = lo
            spill[pl.ds(p.y0 + i, 1), :] = last_y(j)

        rows = pl.ds(c * half * p.y1, half * p.y1)
        z[rows, :] = dot(uhi[rows, :], kz1[...]) + dot(ulo[rows, :], kz1[...])

        @pl.loop(0, half)
        def _(j):
            i = c * half + j
            rows = pl.ds(pl.multiple_of(i * p.y1, p.y1), p.y1)
            plane = z[rows, :]
            dacc[...] += jnp.where(lanes == i, plane[:, LANES:], 0.0)
            hi, lo = halves(plane)
            zhi[rows, :] = hi
            zlo[rows, :] = lo

    put_plane(0, 0.25 * vin[p.nx])
    spill[0 : p.y1, :] = fold_y(0)
    spill[p.c0 : p.c0 + 1, :] = last_y(0)
    shi, slo = halves(spill[...])
    zs = dot(shi, kz1[...]) + dot(slo, kz1[...])
    hi, lo = halves(zs)
    zhi[p.main :, :] = hi
    zlo[p.main :, :] = lo
    tail_one = dot(tail1[...], shi, ((1,), (1,))) + dot(tail1[...], slo, ((1,), (1,)))
    mx1, my1, mxy1, mz1, mxc, myc, mxyc, mzc, m8 = sends
    mx1[...] = zs[0 : p.bx, :LANES]
    my1[...] = zs[p.y0 : p.c0, :LANES]
    mxy1[...] = zs[p.c0 : p.c0 + 8, :LANES]
    mz1[...] = dacc[...]
    pl.semaphore_wait(barrier, len(others))

    rx1, ry1, rxy1, rz1, rxc, ryc, rxyc, rzc, r8 = recvs
    srcs = [mx1, my1, mxy1, mz1, mxc, myc, mxyc, mzc, m8, m8, m8]
    dsts = [rx1, ry1, rxy1, rz1, rxc, ryc, rxyc, rzc, r8.at[0], r8.at[1], r8.at[2]]
    hops = HOPS[:4] + HOPS[:4] + HOPS[4:]
    has_next, has_prev, copies = [], [], []
    for n, hop in enumerate(hops):
        ok_n, target = along(hop, 1)
        has_next.append(ok_n)
        has_prev.append(along(hop, -1)[0])
        copies.append(
            pltpu.make_async_remote_copy(
                src_ref=srcs[n],
                dst_ref=dsts[n],
                send_sem=ssem.at[n],
                recv_sem=rsem.at[n],
                device_id=target,
                device_id_type=MESH,
            )
        )

    def send(which):
        for n in which:

            @pl.when(has_next[n])
            def _():
                copies[n].start()

    send((0, 3, 1, 2))
    for n in range(len(hops)):

        @pl.when(jnp.logical_not(has_prev[n]))
        def _():
            dsts[n][...] = jnp.zeros(dsts[n].shape, jnp.float32)

    for c in bcopies:
        c.wait()
    b = dot(big[...], zhi[...]) + dot(big[...], zlo[...])
    bhi, blo = halves(b)
    cs = dot(bhi, kz[...]) + dot(blo, kz[...])
    tail_c = dot(tails[...], bhi, ((1,), (1,))) + dot(tails[...], blo, ((1,), (1,)))

    mxc[...] = cs[p.own : p.own + p.bx]
    myc[...] = cs[p.own + p.y0 : p.own + p.c0]
    mxyc[...] = cs[p.own + p.c0 : p.own + p.c0 + 8]
    groups = p.own // LANES
    for g in range(groups):
        mzc[8 * g : 8 * g + 8, :] = tail_c[0:8, g * LANES : (g + 1) * LANES]
    m8[...] = tail_one[0:8] + tail_c[0:8, p.own :]
    send((10, 8, 4, 7, 9, 5, 6))

    for n in range(len(hops)):

        @pl.when(has_prev[n])
        def _():
            copies[n].wait_recv()

    lane8 = lax.broadcasted_iota(jnp.int32, (8, LANES), 1)
    g8 = jnp.where(lane8 < p.y0, r8[0], jnp.where(lane8 < p.c0, r8[1], r8[2]))

    def turned(x, where):
        hi, lo = halves(x.T)
        return dot(hi, where) + dot(lo, where)

    f = turned(g8, place[0:8, :])
    xs1 = rx1[...] + f[0 : p.bx, :LANES]
    ys1 = ry1[...] + f[p.y0 : p.c0, :LANES]
    xy1 = rxy1[...] + f[p.c0 : p.c0 + 8, :LANES]
    pieces = [
        rxc[...] + f[0 : p.bx, LANES:],
        ryc[...] + f[p.y0 : p.c0, LANES:],
        rxyc[...] + f[p.c0 : p.c0 + 8, LANES:],
    ]
    if p.c0 + 8 < LANES:
        pieces.append(jnp.zeros((LANES - p.c0 - 8, LANES), jnp.float32))
    whi, wlo = halves(jnp.concatenate(pieces, axis=0))
    c = cs[0 : p.own] + dot(spread[...], whi) + dot(spread[...], wlo)
    c = c + jnp.concatenate(
        [
            turned(rzc[8 * g : 8 * g + 8, :], place[0:8, LANES:])
            for g in range(groups)
        ],
        axis=0,
    )
    outc[...] = c

    first = lanes == 0
    top = lax.broadcasted_iota(jnp.int32, (p.y1, LANES), 0) == 0
    col = rz1[...]
    acc = jnp.zeros((p.y1, LANES), jnp.float32)
    for i in range(p.x1):
        shifted = pltpu.roll(col, (LANES - i) % LANES, 1) if i else col
        plane = z[i * p.y1 : (i + 1) * p.y1, :LANES] + jnp.where(first, shifted, 0.0)
        edge = ys1[i : i + 1, :]
        if i == 0:
            plane = plane + xs1[0 : p.y1]
            edge = edge + xy1[0:1, :]
        plane = plane + jnp.where(top, edge, 0.0)
        out1[i] = plane
        acc = acc + plane * plane
    results = [
        pltpu.make_async_copy(out1, out1_hbm, osem.at[0]),
        pltpu.make_async_copy(outc, outc_hbm, osem.at[1]),
    ]
    mine[0:1, :] = jnp.sum(acc, axis=0, keepdims=True)
    sq = c * c
    lane1 = lax.broadcasted_iota(jnp.int32, (1, LANES), 1)
    row = jnp.zeros((1, LANES), jnp.float32)
    for l in range(LEVELS - 1):
        total = jnp.sum(sq[p.base[l] : p.base[l + 1]], axis=0, keepdims=True)
        row = jnp.where((lane1 >= p.coff[l]) & (lane1 < p.coff[l + 1]), total, row)
    mine[1:2, :] = row

    for c in results:
        c.start()

    pending = [
        pltpu.make_async_remote_copy(
            src_ref=mine,
            dst_ref=parts.at[k + 1],
            send_sem=asend.at[k],
            recv_sem=arecv.at[k],
            device_id=target,
            device_id_type=MESH,
        )
        for k, target in enumerate(others)
    ]
    for c in reversed(pending):
        c.start()
    parts[0] = mine[...]
    for c in pending:
        c.wait_recv()
    stats[...] = jnp.sum(parts[...], axis=0)
    for c in results:
        c.wait()
    for c in pending:
        c.wait_send()
    for n in range(len(hops)):

        @pl.when(has_next[n])
        def _():
            copies[n].wait_send()


def scale_kernel(plan, devices, grid, packed, stats, o1, o2, o3, o4, o5, scales):
    p = plan
    lane1 = lax.broadcasted_iota(jnp.int32, (1, LANES), 1)
    outs = (o1, o2, o3, o4, o5)
    product = jnp.ones((1, 1), jnp.float32)
    for l in range(LEVELS):
        row = stats[0:1, :] if l == 0 else stats[1:2, :]
        if l:
            row = jnp.where(
                (lane1 >= p.coff[l - 1]) & (lane1 < p.coff[l]), row, 0.0
            )
        total = jnp.sum(row, axis=1, keepdims=True)
        cells = devices * (p.nx >> (l + 1)) * (p.ny >> (l + 1)) * (p.nz >> (l + 1))
        scale = jnp.sqrt(total / (product * product) / cells + EPSILON)
        product = product * scale
        scales[l] = scale[0, 0]
        inverse = 1.0 / product
        if l == 0:
            o1[...] = grid[...] * inverse.reshape(1, 1, 1)
            continue
        k = l - 1
        block = packed[p.base[k] : p.base[k + 1], :] * inverse
        if p.coff[k]:
            block = pltpu.roll(block, LANES - p.coff[k], 1)
        block = block.reshape(p.xs[k], p.pys[k], LANES)
        outs[l][...] = block[:, : p.ys[k], : p.zs[k]]


def per_device(sizes, residual_in):
    plan = Plan(residual_in.shape)
    p = plan
    packed_table = p.tables()
    chunks = 4
    count = sizes[0] * sizes[1] * sizes[2]
    f32, bf16 = jnp.float32, jnp.bfloat16
    ends = [(p.bx, LANES), (p.by, LANES), (8, LANES)]
    messages = ends + [(p.y1, LANES)] + ends + [(8 * (p.own // LANES), LANES)]
    anywhere = pl.BlockSpec(memory_space=pl.ANY)
    vmem = pl.BlockSpec(memory_space=pltpu.VMEM)
    dma = pltpu.SemaphoreType.DMA
    grid, packed, stats = pl.pallas_call(
        functools.partial(gather_kernel, p, sizes, chunks),
        out_shape=(
            jax.ShapeDtypeStruct((p.x1, p.y1, p.z1), f32),
            jax.ShapeDtypeStruct((p.own, LANES), f32),
            jax.ShapeDtypeStruct((2, LANES), f32),
        ),
        in_specs=[anywhere] * 2,
        out_specs=(anywhere, anywhere, vmem),
        scratch_shapes=[
            pltpu.VMEM((p.nx + 1, p.ny, p.nz), f32),
            pltpu.VMEM((p.nx // chunks // 2, 2, 8 + p.ny, LANES), f32),
            pltpu.VMEM((LANES, p.nz), f32),
            pltpu.VMEM((p.main, p.nz), bf16),
            pltpu.VMEM((p.main, p.nz), bf16),
            pltpu.VMEM((p.main, 2 * LANES), f32),
            pltpu.VMEM((p.rows1, 2 * LANES), bf16),
            pltpu.VMEM((p.rows1, 2 * LANES), bf16),
            pltpu.VMEM((p.y1, LANES), f32),
        ]
        + [pltpu.VMEM(t, bf16) for t in p.small + [(p.crows, p.rows1)]]
        + [pltpu.VMEM(s, f32) for s in messages + [(8, LANES)]]
        + [pltpu.VMEM(s, f32) for s in messages + [(3, 8, LANES)]]
        + [
            pltpu.VMEM((2, LANES), f32),
            pltpu.VMEM((count, 2, LANES), f32),
            dma((chunks,)),
            dma((6,)),
            dma((-(-p.rows1 // p.nz),)),
            dma((11,)),
            dma((11,)),
            dma((count - 1,)),
            dma((count - 1,)),
            pltpu.VMEM((p.x1, p.y1, p.z1), f32),
            pltpu.VMEM((p.own, LANES), f32),
            dma((2,)),
        ],
        compiler_params=pltpu.CompilerParams(collective_id=0, has_side_effects=True),
        name="restrict_exchange",
    )(residual_in, jnp.asarray(packed_table))
    shapes = [
        (p.nx >> l, p.ny >> l, p.nz >> l) for l in range(1, LEVELS + 1)
    ]
    return pl.pallas_call(
        functools.partial(scale_kernel, p, count),
        out_shape=tuple(jax.ShapeDtypeStruct(s, f32) for s in shapes)
        + (jax.ShapeDtypeStruct((LEVELS,), f32),),
        in_specs=[vmem] * 3,
        out_specs=(vmem,) * 5 + (pl.BlockSpec(memory_space=pltpu.SMEM),),
        name="scale_levels",
    )(grid, packed, stats)


def solution(mesh):
    sizes = tuple(mesh.shape[a] for a in AXES)
    spec = P(*AXES)
    return jax.shard_map(
        functools.partial(per_device, sizes),
        mesh=mesh,
        in_specs=(spec,),
        out_specs=(spec,) * 5 + (P(),),
        check_vma=False,
    )
```
